32 devices in a mesh: fact: 8 (over z, x), dim: 4 (over y, core).
Axes of the slice: x: 2, y: 2, z: 4, core: 2. Of those that a mesh axis runs over, the one named last changes fastest.
Arguments:
- fact_keys: int32 [1048576], P(('fact', 'dim')), may hold values from 0 to 65535, as said below
- revenue: bfloat16 [1048576], P(('fact', 'dim')), may hold values from 0.099609375 to 1
- filter_bits: int32 [256, 256], replicated, may hold values from 0 to 1
- categories: int32 [65536], P(('fact', 'dim')), may hold values from 0 to 511
- attributes: bfloat16 [65536, 128], P(('fact', 'dim')), may hold values from -0.125 to 0.125
Outputs:
- category_totals: float32 [512, 128], P(('fact', 'dim'))
The draws below stay inside these ranges and needn't reach their ends.
Inputs may be any that keep to these rules, and one draw needn't show every extreme that they name: `fact_keys`: keys of owner o are o * 2048 to (o + 1) * 2048 - 1. Among the 32768 rows of one device at most 2048 have keys of any one owner; in every draw one owner gets exactly 2048 matching rows from every device, and every device has exactly 2048 matching rows for some owner.
All inputs are finite; a program needn't handle non-finite values.
Results may differ from the reference program's by a relative error of at most 0.0003.
Values may be sent and summed in bfloat16 or wider, within the bound.
No kernel may reach another device: no remote copies, remote signals or barrier semaphores. Data moves between devices by JAX's collectives and lax.ppermute only.
A program may use at most 64 MiB of HBM per device.

```python
import math
import jax
import jax.numpy as jnp

KEYS = 65536
KEY_LO = 256
KEY_HI = 256
ATTR = 128
CATS = 512
FACT_DEV = 32768
FACT_ROWS = 1048576
KEYS_OWN = 2048
CAP = 2048
N_FACT = 8
N_DIM = 4


def layout(key):
    devices = N_FACT * N_DIM
    first, second, third, fourth = jax.random.split(jax.random.fold_in(key, 7), 4)
    common = jax.random.randint(first, (), 0, devices)
    picked_all = jax.random.randint(second, (devices,), 0, devices)

    def one_device(device_key, picked):
        key_a, key_b, key_c = jax.random.split(device_key, 3)
        slot_owner = jnp.arange(devices * CAP, dtype=jnp.int32) // CAP
        score = jax.random.permutation(key_a, devices * CAP).astype(jnp.int32)
        forced = (slot_owner == common) | (slot_owner == picked)
        score = jnp.where(forced, score - devices * CAP, score)
        order = jnp.argsort(score, stable=True)[:FACT_DEV]
        owners = jax.random.permutation(key_b, slot_owner[order])
        local = jax.random.randint(key_c, (FACT_DEV,), 0, KEYS_OWN)
        is_forced = (owners == common) | (owners == picked)
        return (owners * KEYS_OWN + local, is_forced)
    keys, forced = jax.vmap(one_device)(jax.random.split(third, devices), picked_all)
    levels = jax.random.randint(fourth, (KEYS,), 0, 4)
    bits = (levels > 0).astype(jnp.int32)
    marks = jnp.where(forced, keys, KEYS).reshape(-1)
    bits = bits.at[marks].set(1, mode='drop')
    return (keys.reshape(-1).astype(jnp.int32), bits.reshape(KEY_HI, KEY_LO).astype(jnp.int32))


def draw_fact_keys(key, part):
    return layout(key)[0]


def draw_filter_bits(key, part):
    return layout(key)[1]


def plant(drawn, key, smallest, top_value):
    dims = drawn.shape
    place = [jax.random.randint(jax.random.fold_in(key, axis), (), 0, dims[axis]) for axis in range(len(dims))]
    drawn = drawn.at[tuple(place)].set(smallest)
    longest = dims.index(max(dims))
    place[longest] = (place[longest] + 1) % dims[longest]
    return drawn.at[tuple(place)].set(top_value)


def shard_levels(stream_key, extent, cuts, least, largest):
    def one(dim, blocks):
        draws = jax.random.uniform(jax.random.fold_in(jax.random.fold_in(stream_key, 6), dim), (blocks,), jnp.float32, least / len(cuts), largest / len(cuts))
        return jnp.repeat(jnp.exp(draws), extent[dim] // blocks).reshape((-1,) + (1,) * (len(extent) - dim - 1))

    gain = one(*cuts[0])
    for cut in cuts[1:]:
        gain = gain * one(*cut)
    return gain


def normal_values(key, extent, scale, reach, cuts=(), kind=jnp.bfloat16):
    entries = scale * jax.random.normal(key, extent, jnp.float32)
    if cuts:
        entries = entries * shard_levels(key, extent, cuts, -0.22, 0.18)
    return jnp.clip(entries, -reach, reach).astype(kind)


def setup_inputs(seed: int = 0) -> dict:
    key_of = jax.random.split(jax.random.key(seed), 6)
    fact_keys = draw_fact_keys(jax.random.fold_in(key_of[5], 71), 0)
    revenue = jnp.clip(jnp.exp(math.log(1.0) - 2.306499 * jax.random.uniform(key_of[1], (FACT_ROWS,), jnp.float32) ** shard_levels(key_of[1], (FACT_ROWS,), ((0, 32),), -0.2, 0.2)), 0.099609375, 1.0).astype(jnp.bfloat16)
    filter_bits = draw_filter_bits(jax.random.fold_in(key_of[5], 71), 0)
    categories = plant(jax.random.randint(key_of[3], (KEYS,), 0, CATS), jax.random.fold_in(key_of[3], 1), 0, CATS - 1).astype(jnp.int32)
    attributes = normal_values(key_of[4], (KEYS, ATTR), (FACT_DEV * N_FACT * N_DIM // CATS) ** -0.5, 0.125, ((0, 32),))
    return dict(fact_keys=fact_keys, revenue=revenue, filter_bits=filter_bits, categories=categories, attributes=attributes)


def reference(fact_keys, revenue, filter_bits, categories, attributes):
    match = filter_bits.reshape(-1)[fact_keys]
    weight = jnp.where(match == 1, revenue.astype(jnp.float32), jnp.float32(0.0))
    key_revenue = jax.ops.segment_sum(weight, fact_keys, num_segments=KEYS)
    weighted = key_revenue[:, None] * attributes.astype(jnp.float32)
    return jax.ops.segment_sum(weighted, categories, num_segments=CATS)
```

```python
import jax
import jax.numpy as jnp
from jax import lax
from jax.experimental import pallas as pl
from jax.experimental.pallas import tpu as pltpu
from jax.sharding import PartitionSpec as P

CATS = 512
AXES = ("fact", "dim")
LANES = 128
SUB = 16
CHUNK = 16


def hot(values, size):
    iota = lax.broadcasted_iota(jnp.int32, (size // SUB, SUB, LANES), 0) * SUB
    iota = iota + lax.broadcasted_iota(jnp.int32, (size // SUB, SUB, LANES), 1)
    iota = iota.astype(jnp.float32).astype(jnp.bfloat16)
    row = jnp.broadcast_to(values, (SUB, LANES)).astype(jnp.float32).astype(jnp.bfloat16)
    return iota == row[None]


def key_kernel(keys_ref, rev_ref, out_ref):
    groups = keys_ref.shape[0]
    key_hi, key_lo = out_ref.shape
    out_ref[...] = jnp.zeros_like(out_ref)
    one = jnp.ones((), jnp.bfloat16)
    zero = jnp.zeros((), jnp.bfloat16)

    def body(g, carry):
        base = pl.multiple_of(g * CHUNK, CHUNK)
        keys = keys_ref[pl.ds(base, CHUNK), :]
        rev = rev_ref[pl.ds(base, CHUNK), :].astype(jnp.float32)
        high = keys // key_lo
        low = keys % key_lo
        lhs, rhs = [], []
        for j in range(CHUNK):
            lhs.append(
                jnp.where(hot(high[j : j + 1], key_hi), one, zero).reshape(key_hi, LANES)
            )
            row = jnp.broadcast_to(rev[j : j + 1], (SUB, LANES)).astype(jnp.bfloat16)
            rhs.append(
                jnp.where(hot(low[j : j + 1], key_lo), row[None], zero).reshape(key_lo, LANES)
            )
        out_ref[...] += lax.dot_general(
            jnp.concatenate(lhs, axis=1),
            jnp.concatenate(rhs, axis=1),
            (((1,), (1,)), ((), ())),
            preferred_element_type=jnp.float32,
        )
        return carry

    lax.fori_loop(0, groups // CHUNK, body, 0)


def key_sums(fact_keys, revenue, key_hi, key_lo):
    vmem = pl.BlockSpec(memory_space=pltpu.VMEM)
    return pl.pallas_call(
        key_kernel,
        in_specs=[vmem, vmem],
        out_specs=vmem,
        out_shape=jax.ShapeDtypeStruct((key_hi, key_lo), jnp.float32),
        name="key_sums",
    )(fact_keys.reshape(-1, LANES), revenue.reshape(-1, LANES))


def category_kernel(terms_ref, filt_ref, cats_ref, attrs_ref, out_ref):
    half = out_ref.shape[0] // 2
    cats = cats_ref[...]
    sums = jnp.where(filt_ref[...] == 1, jnp.sum(terms_ref[...], axis=0), 0.0)
    coarse = sums.astype(jnp.bfloat16).astype(jnp.float32)
    fine = sums - coarse
    zero = jnp.zeros((), jnp.bfloat16)
    parts = sums.shape[1] // LANES
    for part in range(2):
        lhs, rhs = [], []
        for j in range(cats.shape[0]):
            r, c = j // parts, (j % parts) * LANES
            mask = hot(cats[j : j + 1] - part * half, half)
            attrs = attrs_ref[j * LANES : (j + 1) * LANES, :]
            for piece in (coarse, fine):
                row = jnp.broadcast_to(piece[r : r + 1, c : c + LANES], (SUB, LANES))
                row = row.astype(jnp.bfloat16)[None]
                lhs.append(jnp.where(mask, row, zero).reshape(half, LANES))
                rhs.append(attrs)
        out_ref[part * half : (part + 1) * half, :] = jnp.dot(
            jnp.concatenate(lhs, axis=1),
            jnp.concatenate(rhs, axis=0),
            preferred_element_type=jnp.float32,
        )


def category_sums(terms, filt, categories, attributes):
    vmem = pl.BlockSpec(memory_space=pltpu.VMEM)
    return pl.pallas_call(
        category_kernel,
        in_specs=[vmem, vmem, vmem, vmem],
        out_specs=vmem,
        out_shape=jax.ShapeDtypeStruct((CATS, attributes.shape[1]), jnp.float32),
        name="category_sums",
    )(terms, filt, categories.reshape(-1, LANES), attributes)


def solution(mesh):
    devices = mesh.shape["fact"] * mesh.shape["dim"]

    def spread(partial):
        blocks = partial.reshape(devices, -1, partial.shape[1])
        return lax.all_to_all(blocks, AXES, 0, 0, tiled=True)

    def per_device(fact_keys, revenue, filter_bits, categories, attributes):
        key_hi, key_lo = filter_bits.shape
        terms = spread(key_sums(fact_keys, revenue, key_hi, key_lo))
        rows = terms.shape[1]
        filt = lax.dynamic_slice_in_dim(filter_bits, lax.axis_index(AXES) * rows, rows, 0)
        partial = category_sums(terms, filt, categories, attributes)
        return jnp.sum(spread(partial), axis=0)

    in_specs = (P(AXES), P(AXES), P(), P(AXES), P(AXES, None))
    return jax.shard_map(
        per_device, mesh=mesh, in_specs=in_specs, out_specs=P(AXES, None), check_vma=False
    )
```

```python
import jax
import jax.numpy as jnp
from jax import lax
from jax.experimental import pallas as pl
from jax.experimental.pallas import tpu as pltpu
from jax.sharding import PartitionSpec as P

CATS = 512
AXES = ("fact", "dim")
LANES = 128
SUB = 16
CHUNK = 128


def hot(values, size):
    iota = lax.broadcasted_iota(jnp.int32, (size // SUB, SUB, LANES), 0) * SUB
    iota = iota + lax.broadcasted_iota(jnp.int32, (size // SUB, SUB, LANES), 1)
    iota = iota.astype(jnp.float32).astype(jnp.bfloat16)
    row = jnp.broadcast_to(values, (SUB, LANES)).astype(jnp.float32).astype(jnp.bfloat16)
    return iota == row[None]


def key_kernel(keys_ref, rev_ref, out_ref):
    groups = keys_ref.shape[0]
    key_hi, key_lo = out_ref.shape
    out_ref[...] = jnp.zeros_like(out_ref)
    one = jnp.ones((), jnp.bfloat16)
    zero = jnp.zeros((), jnp.bfloat16)

    def body(g, carry):
        base = pl.multiple_of(g * CHUNK, CHUNK)
        keys = keys_ref[pl.ds(base, CHUNK), :]
        rev = rev_ref[pl.ds(base, CHUNK), :].astype(jnp.float32)
        high = keys // key_lo
        low = keys % key_lo
        lhs, rhs = [], []
        for j in range(CHUNK):
            lhs.append(
                jnp.where(hot(high[j : j + 1], key_hi), one, zero).reshape(key_hi, LANES)
            )
            row = jnp.broadcast_to(rev[j : j + 1], (SUB, LANES)).astype(jnp.bfloat16)
            rhs.append(
                jnp.where(hot(low[j : j + 1], key_lo), row[None], zero).reshape(key_lo, LANES)
            )
        out_ref[...] += lax.dot_general(
            jnp.concatenate(lhs, axis=1),
            jnp.concatenate(rhs, axis=1),
            (((1,), (1,)), ((), ())),
            preferred_element_type=jnp.float32,
        )
        return carry

    lax.fori_loop(0, groups // CHUNK, body, 0)


def key_sums(fact_keys, revenue, key_hi, key_lo):
    vmem = pl.BlockSpec(memory_space=pltpu.VMEM)
    return pl.pallas_call(
        key_kernel,
        in_specs=[vmem, vmem],
        out_specs=vmem,
        out_shape=pltpu.VMEM((key_hi, key_lo), jnp.float32),
        name="key_sums",
    )(fact_keys.reshape(-1, LANES), revenue.reshape(-1, LANES))


def category_kernel(terms_ref, filt_ref, cats_ref, attrs_ref, out_ref):
    size, width = out_ref.shape
    half = size // 2
    cats = cats_ref[...]
    sums = jnp.where(filt_ref[...] == 1, jnp.sum(terms_ref[...], axis=0), 0.0)
    parts = sums.shape[1] // LANES
    one = jnp.ones((), jnp.bfloat16)
    zero = jnp.zeros((), jnp.bfloat16)
    lhs, rhs = [], []
    for j in range(cats.shape[0]):
        r, c = j // parts, (j % parts) * LANES
        masks = [hot(cats[j : j + 1] - part * half, half) for part in range(2)]
        lhs.append(
            jnp.concatenate([jnp.where(m, one, zero).reshape(half, LANES) for m in masks], axis=0)
        )
        column = jnp.broadcast_to(sums[r : r + 1, c : c + LANES], (LANES, LANES)).T
        attrs = attrs_ref[j * LANES : (j + 1) * LANES, :].astype(jnp.float32)
        weighted = column * attrs
        coarse = weighted.astype(jnp.bfloat16)
        fine = (weighted - coarse.astype(jnp.float32)).astype(jnp.bfloat16)
        rhs.append(jnp.concatenate([coarse, fine], axis=1))
    both = jnp.dot(
        jnp.concatenate(lhs, axis=1),
        jnp.concatenate(rhs, axis=0),
        preferred_element_type=jnp.float32,
    )
    out_ref[...] = both[:, :width] + both[:, width:]


def category_sums(terms, filt, categories, attributes):
    args = (terms, filt, categories.reshape(-1, LANES), attributes)
    vmem = pl.BlockSpec(memory_space=pltpu.VMEM)
    return pl.pallas_call(
        category_kernel,
        in_specs=[vmem, vmem, vmem, vmem],
        out_specs=vmem,
        out_shape=pltpu.VMEM((CATS, attributes.shape[1]), jnp.float32),
        name="category_sums",
    )(*(pltpu.with_memory_space_constraint(x, pltpu.VMEM) for x in args))


def solution(mesh):
    devices = mesh.shape["fact"] * mesh.shape["dim"]

    def spread(partial):
        blocks = partial.reshape(devices, -1, partial.shape[1])
        return lax.all_to_all(blocks, AXES, 0, 0, tiled=True)

    def per_device(fact_keys, revenue, filter_bits, categories, attributes):
        key_hi, key_lo = filter_bits.shape
        terms = spread(key_sums(fact_keys, revenue, key_hi, key_lo))
        rows = terms.shape[1]
        filt = lax.dynamic_slice_in_dim(filter_bits, lax.axis_index(AXES) * rows, rows, 0)
        partial = category_sums(terms, filt, categories, attributes)
        return jnp.sum(spread(partial), axis=0)

    in_specs = (P(AXES), P(AXES), P(), P(AXES), P(AXES, None))
    return jax.shard_map(
        per_device, mesh=mesh, in_specs=in_specs, out_specs=P(AXES, None), check_vma=False
    )
```
